512 devices in a mesh: grp: 16 (over z, core), shard: 32 (over x, y).
Axes of the slice: x: 4, y: 8, z: 8, core: 2. Of those that a mesh axis runs over, the one named last changes fastest.
Arguments:
- partial_grads: bfloat16 [16, 4096, 6144], P('grp', 'shard')
- joined_block: int32 [48], replicated, may hold values from 0 to 47, each once
- head_slot: int32 [48], replicated, may hold values from 0 to 63, as said below
Outputs:
- head_grads: float32 [64, 32, 128, 128], P('shard', None, 'grp')
- head_rms: float32 [64], P('shard')
- type_rms: float32 [3], replicated
The draws below stay inside these ranges and needn't reach their ends.
Inputs may be any that keep to these rules, and one draw needn't show every extreme that they name: `joined_block`: a permutation: each block number appears once. `head_slot`: distinct slots; every owner along shard holds 2 or 1 head blocks, and some owner holds 2.
All inputs are finite; a program needn't handle non-finite values.
Results may differ from the reference program's by a relative error of at most 0.0003.
Values may be sent and summed in bfloat16 or wider, within the bound.
No kernel may reach another device: no remote copies, remote signals or barrier semaphores. Data moves between devices by JAX's collectives and lax.ppermute only.
A program may use at most 64 MiB of HBM per device.

```python
import jax
import jax.numpy as jnp
from jax import lax

D = 4096
QH = 32
KVH = 8
HS = 128
BLOCKS = 48
COLS = 6144
SLOTS_DEV = 2
SLOTS = 64
N_GRP = 16
N_SHARD = 32


def draw_partial_grads(key, part):
    row_index = jnp.arange(D)
    block_pos = (row_index % (D // N_SHARD)).astype(jnp.float32) / (D // N_SHARD)
    rise = jnp.exp(jnp.log(3.0) * block_pos)
    row_scale = jnp.exp(jax.random.uniform(jax.random.fold_in(key, 11), (D,), jnp.float32, 0.0, jnp.log(10.0))) * rise
    col_scale = jnp.exp(jax.random.uniform(jax.random.fold_in(key, 12), (COLS,), jnp.float32, 0.0, jnp.log(10.0)))
    overall = 0.01

    def draw_group(group):
        noise = jax.random.normal(jax.random.fold_in(jax.random.fold_in(key, 14), group), (D, COLS), jnp.float32)
        return (noise * row_scale[:, None] * col_scale[None, :] * overall).astype(jnp.bfloat16)
    return lax.map(draw_group, jnp.arange(N_GRP))


def draw_head_slot(key, part):
    slot_total = SLOTS_DEV * N_SHARD
    empty_count = slot_total - BLOCKS
    owners = jax.random.permutation(jax.random.fold_in(key, 21), N_SHARD).astype(jnp.int32)
    lost_pos = jax.random.randint(jax.random.fold_in(key, 22), (N_SHARD,), 0, SLOTS_DEV).astype(jnp.int32)
    lost_slot = owners * SLOTS_DEV + lost_pos
    chosen = jnp.arange(N_SHARD, dtype=jnp.int32) < empty_count
    slot_ids = jnp.arange(slot_total, dtype=jnp.int32)
    dead_slot = jnp.any((slot_ids[:, None] == lost_slot[None, :]) & chosen[None, :], axis=1)
    sort_keys = dead_slot.astype(jnp.int32) * slot_total + slot_ids
    live_slots = jnp.argsort(sort_keys).astype(jnp.int32)[:BLOCKS]
    shuffle = jax.random.permutation(jax.random.fold_in(key, 23), BLOCKS).astype(jnp.int32)
    return live_slots[shuffle].astype(jnp.int32)


def setup_inputs(seed: int = 0) -> dict:
    streams_of = jax.random.split(jax.random.key(seed), 4)
    return {
        "partial_grads": draw_partial_grads(jax.random.fold_in(streams_of[3], 71), 0),
        "joined_block": jax.random.permutation(streams_of[1], BLOCKS).astype(jnp.int32),
        "head_slot": draw_head_slot(jax.random.fold_in(streams_of[3], 71), 0),
    }


def reference(partial_grads, joined_block, head_slot):

    def add_group(carry, group_term):
        return (carry + group_term.astype(jnp.float32), None)
    reduced, _ = lax.scan(add_group, jnp.zeros((D, COLS), jnp.float32), partial_grads)
    block_ids = jnp.arange(BLOCKS, dtype=jnp.int32)
    block_kind = (block_ids >= QH).astype(jnp.int32) + (block_ids >= QH + KVH).astype(jnp.int32)
    matches = (head_slot[None, :] == jnp.arange(SLOTS, dtype=jnp.int32)[:, None]).astype(jnp.int32)
    occupied = lax.optimization_barrier(jnp.sum(matches, axis=1))
    source = lax.optimization_barrier(jnp.sum(matches * joined_block[None, :], axis=1)).astype(jnp.int32)
    slot_kind = lax.optimization_barrier(jnp.sum(matches * block_kind[None, :], axis=1)) + (1 - occupied) * 3
    picked = jnp.take(reduced.reshape(D, BLOCKS, HS), source, axis=1)
    picked = picked * occupied.astype(jnp.float32)[None, :, None]
    head_grads = jnp.transpose(picked, (1, 0, 2)).reshape(SLOTS, N_SHARD, D // N_SHARD, HS)
    squares = lax.optimization_barrier(jnp.sum(head_grads * head_grads, axis=(1, 2, 3)))
    head_rms = jnp.sqrt(squares / (D * HS))
    selector = (slot_kind[:, None] == jnp.arange(3, dtype=jnp.int32)[None, :]).astype(jnp.float32)
    type_squares = lax.optimization_barrier(jnp.sum(squares[:, None] * selector, axis=0))
    counts = jnp.array([QH, KVH, KVH], jnp.float32) * (D * HS)
    type_rms = jnp.sqrt(type_squares / counts)
    return (head_grads, head_rms, type_rms)
```

```python
import jax
import jax.numpy as jnp
from jax import lax
from jax.sharding import Mesh
from jax.sharding import PartitionSpec as P

D = 4096
QH = 32
KVH = 8
HS = 128
SHARD = ("shard_0", "shard_1")
GRP = ("grp_0", "grp_1")


def over_copies(row, axes):
    copies = jnp.broadcast_to(row, (lax.axis_size(axes), *row.shape))
    return lax.all_to_all(copies, axes, split_axis=0, concat_axis=0, tiled=True).sum(axis=0)


def per_device(partial_grads, joined_block, head_slot):
    own_rows = partial_grads[0]
    blocks = joined_block.shape[0]
    groups = lax.axis_size(GRP)
    width = own_rows.shape[1]
    rows = own_rows.shape[0] // groups
    shard_count = lax.axis_size(SHARD)
    slots_dev = (blocks + shard_count - 1) // shard_count
    slot_total = slots_dev * shard_count
    first_slot = lax.axis_index(SHARD) * slots_dev

    parts = lax.all_to_all(own_rows.reshape(groups, rows, width), GRP, 0, 0, tiled=True)
    summed = jnp.sum(parts.astype(jnp.float32), axis=0)

    by_block = summed.reshape(rows, blocks, HS)
    squares = jnp.sum(by_block * by_block, axis=(0, 2))
    square_tile = jnp.pad(squares[None], ((0, rows - 1), (0, HS - blocks)))

    block_ids = jnp.arange(blocks, dtype=jnp.int32)
    slot_ids = jnp.arange(slot_total, dtype=jnp.int32)
    matches = (head_slot[None, :] == slot_ids[:, None]).astype(jnp.int32)
    occupied = jnp.sum(matches, axis=1)
    source = jnp.sum(matches * joined_block[None, :], axis=1)
    picked = jnp.take(by_block, source, axis=1)
    picked = jnp.where(occupied[None, :, None] > 0, picked, jnp.zeros_like(picked))
    tiles = jnp.transpose(picked, (1, 0, 2)).reshape(shard_count, slots_dev, rows, HS)
    riders = jnp.broadcast_to(square_tile, (shard_count, 1, rows, HS))
    arrived = lax.all_to_all(
        jnp.concatenate([tiles, riders], axis=1), SHARD, split_axis=0, concat_axis=0, tiled=True
    )
    owned_block = jnp.transpose(arrived[:, :slots_dev], (1, 0, 2, 3))
    shard_squares = arrived[:, slots_dev, :1].sum(axis=0)

    every_square = over_copies(shard_squares, GRP)[0, :blocks]
    kind = (block_ids >= QH).astype(jnp.int32) + (block_ids >= QH + KVH).astype(jnp.int32)
    own = head_slot[None, :] == first_slot + jnp.arange(slots_dev, dtype=jnp.int32)[:, None]
    alike = kind[None, :] == jnp.arange(3, dtype=jnp.int32)[:, None]
    wanted = jnp.concatenate([own, alike], axis=0)
    joined = joined_block[:, None] == block_ids[None, :]
    chosen = jnp.any(wanted[:, :, None] & joined[None], axis=1).astype(jnp.float32)
    sums = jnp.sum(chosen * every_square[None, :], axis=1)
    head_rms = jnp.sqrt(sums[:slots_dev] / (D * HS))
    counts = jnp.array([QH, KVH, KVH], jnp.float32) * (D * HS)
    type_rms = jnp.sqrt(sums[slots_dev:] / counts)
    return (owned_block, head_rms, type_rms)


def solution(mesh):
    finer = Mesh(mesh.devices.reshape(8, 2, 4, 8), ("grp_0", "grp_1", "shard_0", "shard_1"))
    in_specs = (P(GRP, SHARD, None), P(), P())
    out_specs = (P(SHARD, None, GRP, None), P(SHARD), P())
    return jax.shard_map(
        per_device, mesh=finer, in_specs=in_specs, out_specs=out_specs, check_vma=False
    )
```

```python
import functools

import jax
import jax.numpy as jnp
from jax import lax
from jax.experimental import pallas as pl
from jax.experimental.pallas import tpu as pltpu
from jax.sharding import Mesh
from jax.sharding import PartitionSpec as P

D = 4096
QH = 32
KVH = 8
HS = 128
SHARD = ("shard_0", "shard_1")
GRP = ("grp_0", "grp_1")
IN_VMEM = pl.BlockSpec(memory_space=pltpu.VMEM)
PARAMS = pltpu.CompilerParams(vmem_limit_bytes=4 * 2**20)
IN_SMEM = pl.BlockSpec(memory_space=pltpu.SMEM)


def outgoing_body(peers, per_peer, source_ref, occupied_ref, summed_ref, out_ref):
    rows = summed_ref.shape[0]
    stride = per_peer * rows + 1
    slot_rows = []
    for slot in range(peers * per_peer):
        first = pl.multiple_of(source_ref[slot] * HS, HS)
        tile = summed_ref[:, pl.ds(first, HS)]
        tile = jnp.where(occupied_ref[slot] > 0, tile, jnp.zeros_like(tile))
        peer, nth = divmod(slot, per_peer)
        out_ref[pl.ds(peer * stride + nth * rows, rows), :] = tile
        slot_rows.append(jnp.sum(tile * tile, axis=0, keepdims=True))
    squares = jnp.sum(jnp.concatenate(slot_rows, axis=0), axis=1, keepdims=True)
    shape = (peers * per_peer, HS)
    here = lax.broadcasted_iota(jnp.int32, shape, 0) == lax.broadcasted_iota(jnp.int32, shape, 1)
    rider = jnp.sum(jnp.where(here, squares, 0.0), axis=0, keepdims=True)
    for peer in range(peers):
        out_ref[pl.ds(peer * stride + stride - 1, 1), :] = rider


def riders_body(peers, stride, copies, arrived_ref, out_ref):
    total = arrived_ref[pl.ds(stride - 1, 1), :]
    for peer in range(1, peers):
        total = total + arrived_ref[pl.ds(peer * stride + stride - 1, 1), :]
    out_ref[...] = jnp.broadcast_to(total, (copies, HS))


def owned_body(peers, per_peer, rows, arrived_ref, out_ref):
    stride = per_peer * rows + 1
    for peer in range(peers):
        for nth in range(per_peer):
            out_ref[nth, peer] = arrived_ref[pl.ds(peer * stride + nth * rows, rows), :]


def per_device(partial_grads, joined_block, head_slot):
    own_rows = partial_grads[0]
    blocks = joined_block.shape[0]
    groups = lax.axis_size(GRP)
    width = own_rows.shape[1]
    rows = own_rows.shape[0] // groups
    peers = lax.axis_size(SHARD)
    per_peer = (blocks + peers - 1) // peers
    slot_total = per_peer * peers
    first_slot = lax.axis_index(SHARD) * per_peer
    stride = per_peer * rows + 1

    block_ids = jnp.arange(blocks, dtype=jnp.int32)
    slot_ids = jnp.arange(slot_total, dtype=jnp.int32)
    matches = (head_slot[None, :] == slot_ids[:, None]).astype(jnp.int32)
    occupied = jnp.sum(matches, axis=1)
    source = jnp.sum(matches * joined_block[None, :], axis=1)
    block_kind = (block_ids >= QH).astype(jnp.int32) + (block_ids >= QH + KVH).astype(jnp.int32)
    slot_kind = jnp.sum(matches * block_kind[None, :], axis=1) + (1 - occupied) * 3
    own = slot_ids[None, :] == first_slot + jnp.arange(per_peer, dtype=jnp.int32)[:, None]
    alike = slot_kind[None, :] == jnp.arange(3, dtype=jnp.int32)[:, None]

    parts = lax.all_to_all(own_rows.reshape(groups, rows, width), GRP, 0, 0, tiled=True)
    summed = jnp.sum(parts.astype(jnp.float32), axis=0)

    outgoing = pl.pallas_call(
        functools.partial(outgoing_body, peers, per_peer),
        out_shape=jax.ShapeDtypeStruct((peers * stride, HS), jnp.float32),
        in_specs=[IN_SMEM, IN_SMEM, IN_VMEM],
        out_specs=IN_VMEM,
        compiler_params=PARAMS,
    )(source, occupied, summed)
    arrived = lax.all_to_all(outgoing[:, None], SHARD, split_axis=0, concat_axis=0, tiled=True)
    arrived = arrived[:, 0]
    riders = pl.pallas_call(
        functools.partial(riders_body, peers, stride, groups),
        out_shape=jax.ShapeDtypeStruct((groups, HS), jnp.float32),
        in_specs=[IN_VMEM],
        out_specs=IN_VMEM,
        compiler_params=PARAMS,
    )(arrived)
    every = lax.all_to_all(riders[:, None], GRP, split_axis=0, concat_axis=0, tiled=True)
    owned_block = pl.pallas_call(
        functools.partial(owned_body, peers, per_peer, rows),
        out_shape=jax.ShapeDtypeStruct((per_peer, peers, rows, HS), jnp.float32),
        in_specs=[IN_VMEM],
        out_specs=IN_VMEM,
        compiler_params=PARAMS,
        cost_estimate=pl.CostEstimate(flops=10**6, bytes_accessed=2**19, transcendentals=0),
    )(arrived)

    every_square = every.sum(axis=(0, 1))[:slot_total]
    wanted = jnp.concatenate([own, alike], axis=0).astype(jnp.float32)
    sums = jnp.sum(wanted * every_square[None, :], axis=1)
    head_rms = jnp.sqrt(sums[:per_peer] / (D * HS))
    counts = jnp.array([QH, KVH, KVH], jnp.float32) * (D * HS)
    type_rms = jnp.sqrt(sums[per_peer:] / counts)
    return (owned_block, head_rms, type_rms)


def solution(mesh):
    finer = Mesh(mesh.devices.reshape(8, 2, 4, 8), ("grp_0", "grp_1", "shard_0", "shard_1"))
    in_specs = (P(GRP, SHARD, None), P(), P())
    out_specs = (P(SHARD, None, GRP, None), P(SHARD), P())
    return jax.shard_map(
        per_device, mesh=finer, in_specs=in_specs, out_specs=out_specs, check_vma=False
    )
```

```python
import functools

import jax
import jax.numpy as jnp
from jax import lax
from jax.experimental import pallas as pl
from jax.experimental.pallas import tpu as pltpu
from jax.sharding import Mesh
from jax.sharding import PartitionSpec as P

D = 4096
QH = 32
KVH = 8
HS = 128
SHARD = ("shard_0", "shard_1")
GRP = ("grp_0", "grp_1")
IN_VMEM = pl.BlockSpec(memory_space=pltpu.VMEM)
PARAMS = pltpu.CompilerParams(vmem_limit_bytes=4 * 2**20)
IN_SMEM = pl.BlockSpec(memory_space=pltpu.SMEM)


def diagonal_row(rows):
    sums = jnp.sum(rows, axis=1, keepdims=True)
    shape = rows.shape
    here = lax.broadcasted_iota(jnp.int32, shape, 0) == lax.broadcasted_iota(jnp.int32, shape, 1)
    return jnp.sum(jnp.where(here, sums, 0.0), axis=0, keepdims=True)


def squares_body(blocks, summed_ref, out_ref):
    block_rows = []
    for block in range(blocks):
        tile = summed_ref[:, pl.ds(block * HS, HS)]
        block_rows.append(jnp.sum(tile * tile, axis=0, keepdims=True))
    out_ref[...] = jnp.broadcast_to(diagonal_row(jnp.concatenate(block_rows, axis=0)), out_ref.shape)


def outgoing_body(peers, per_peer, source_ref, occupied_ref, summed_ref, squares_ref, out_ref):
    rows = summed_ref.shape[0]
    stride = per_peer * rows + 1
    rider = jnp.sum(squares_ref[...], axis=0, keepdims=True)
    for slot in range(peers * per_peer):
        first = pl.multiple_of(source_ref[slot] * HS, HS)
        tile = summed_ref[:, pl.ds(first, HS)]
        tile = jnp.where(occupied_ref[slot] > 0, tile, jnp.zeros_like(tile))
        peer, nth = divmod(slot, per_peer)
        out_ref[pl.ds(peer * stride + nth * rows, rows), :] = tile
    for peer in range(peers):
        out_ref[pl.ds(peer * stride + stride - 1, 1), :] = rider


def arrived_body(peers, per_peer, rows, arrived_ref, wanted_ref, owned_ref, head_ref, type_ref):
    stride = per_peer * rows + 1
    total = arrived_ref[pl.ds(stride - 1, 1), :]
    for peer in range(1, peers):
        total = total + arrived_ref[pl.ds(peer * stride + stride - 1, 1), :]
    sums = jnp.sum(wanted_ref[...] * total, axis=1, keepdims=True)
    row = lax.broadcasted_iota(jnp.int32, sums.shape, 0)
    heads = jnp.where(row < per_peer, 1, jnp.where(row == per_peer, QH, KVH))
    rms = jnp.sqrt(sums / (heads.astype(jnp.float32) * (D * HS)))
    for nth in range(per_peer):
        head_ref[nth] = jnp.sum(jnp.where(row == nth, rms, 0.0))
    for kind in range(3):
        type_ref[kind] = jnp.sum(jnp.where(row == per_peer + kind, rms, 0.0))
    for peer in range(peers):
        for nth in range(per_peer):
            owned_ref[nth, peer] = arrived_ref[pl.ds(peer * stride + nth * rows, rows), :]


def per_device(partial_grads, joined_block, head_slot):
    own_rows = partial_grads[0]
    blocks = joined_block.shape[0]
    groups = lax.axis_size(GRP)
    width = own_rows.shape[1]
    rows = own_rows.shape[0] // groups
    peers = lax.axis_size(SHARD)
    per_peer = (blocks + peers - 1) // peers
    slot_total = per_peer * peers
    first_slot = lax.axis_index(SHARD) * per_peer
    stride = per_peer * rows + 1

    block_ids = jnp.arange(blocks, dtype=jnp.int32)
    slot_ids = jnp.arange(slot_total, dtype=jnp.int32)
    matches = (head_slot[None, :] == slot_ids[:, None]).astype(jnp.int32)
    occupied = jnp.sum(matches, axis=1)
    source = jnp.sum(matches * joined_block[None, :], axis=1)
    block_kind = (block_ids >= QH).astype(jnp.int32) + (block_ids >= QH + KVH).astype(jnp.int32)
    own = head_slot[None, :] == first_slot + jnp.arange(per_peer, dtype=jnp.int32)[:, None]
    alike = block_kind[None, :] == jnp.arange(3, dtype=jnp.int32)[:, None]
    asked = jnp.concatenate([own, alike], axis=0)
    joined = joined_block[:, None] == block_ids[None, :]
    wanted = jnp.any(asked[:, :, None] & joined[None], axis=1).astype(jnp.float32)
    wanted = jnp.pad(wanted, ((0, 8 - wanted.shape[0]), (0, HS - blocks)))

    parts = lax.all_to_all(own_rows.reshape(groups, rows, width), GRP, 0, 0, tiled=True)
    summed = jnp.sum(parts.astype(jnp.float32), axis=0)

    squares = pl.pallas_call(
        functools.partial(squares_body, blocks),
        out_shape=jax.ShapeDtypeStruct((groups, HS), jnp.float32),
        in_specs=[IN_VMEM],
        out_specs=IN_VMEM,
        compiler_params=PARAMS,
    )(summed)
    squares = lax.all_to_all(squares[:, None], GRP, split_axis=0, concat_axis=0, tiled=True)[:, 0]
    outgoing = pl.pallas_call(
        functools.partial(outgoing_body, peers, per_peer),
        out_shape=jax.ShapeDtypeStruct((peers * stride, HS), jnp.float32),
        in_specs=[IN_SMEM, IN_SMEM, IN_VMEM, IN_VMEM],
        out_specs=IN_VMEM,
        compiler_params=PARAMS,
    )(source, occupied, summed, squares)
    arrived = lax.all_to_all(outgoing[:, None], SHARD, split_axis=0, concat_axis=0, tiled=True)
    return pl.pallas_call(
        functools.partial(arrived_body, peers, per_peer, rows),
        out_shape=(
            jax.ShapeDtypeStruct((per_peer, peers, rows, HS), jnp.float32),
            jax.ShapeDtypeStruct((per_peer,), jnp.float32),
            jax.ShapeDtypeStruct((3,), jnp.float32),
        ),
        in_specs=[IN_VMEM, IN_VMEM],
        out_specs=(IN_VMEM, IN_SMEM, IN_SMEM),
        compiler_params=PARAMS,
    )(arrived[:, 0], wanted)


def solution(mesh):
    finer = Mesh(mesh.devices.reshape(8, 2, 4, 8), ("grp_0", "grp_1", "shard_0", "shard_1"))
    in_specs = (P(GRP, SHARD, None), P(), P())
    out_specs = (P(SHARD, None, GRP, None), P(SHARD), P())
    return jax.shard_map(
        per_device, mesh=finer, in_specs=in_specs, out_specs=out_specs, check_vma=False
    )
```

```python
import functools

import jax
import jax.numpy as jnp
from jax import lax
from jax.experimental import pallas as pl
from jax.experimental.pallas import tpu as pltpu
from jax.sharding import Mesh
from jax.sharding import PartitionSpec as P

D = 4096
QH = 32
KVH = 8
HS = 128
SHARD = ("shard_0", "shard_1")
GRP = ("grp_0", "grp_1")
SCALES = 64
IN_VMEM = pl.BlockSpec(memory_space=pltpu.VMEM)
PARAMS = pltpu.CompilerParams(vmem_limit_bytes=4 * 2**20)
IN_SMEM = pl.BlockSpec(memory_space=pltpu.SMEM)


def diagonal_row(rows):
    sums = jnp.sum(rows, axis=1, keepdims=True)
    shape = rows.shape
    here = lax.broadcasted_iota(jnp.int32, shape, 0) == lax.broadcasted_iota(jnp.int32, shape, 1)
    return jnp.sum(jnp.where(here, sums, 0.0), axis=0, keepdims=True)


def squares_body(blocks, summed_ref, out_ref):
    block_rows = []
    for block in range(blocks):
        tile = summed_ref[:, pl.ds(block * HS, HS)]
        block_rows.append(jnp.sum(tile * tile, axis=0, keepdims=True))
    out_ref[...] = jnp.broadcast_to(diagonal_row(jnp.concatenate(block_rows, axis=0)), out_ref.shape)


def halves(exponent):
    return jnp.exp2(exponent * 0.5)


def words_of(values):
    exponent = jnp.floor(jnp.log2(jnp.maximum(values, 1e-37)))
    down = halves(-exponent)
    mantissa = jnp.floor(values * down * down * 2.0**18).astype(jnp.int32) + 1
    return jnp.where(values > 0.0, mantissa * 1024 + exponent.astype(jnp.int32) + 512, 0), exponent


def mantissa_of(words):
    return (words >> 10).astype(jnp.float32) * 2.0**-18


def exponent_of(words):
    return ((words & 1023) - 512).astype(jnp.float32)


def code_tile(tile, first_lane):
    most = jnp.max(jnp.abs(tile), axis=1, keepdims=True)
    words, exponent = words_of(most)
    down = halves(-exponent)
    gain = 32767.0 / jnp.where(words > 0, mantissa_of(words), 1.0)
    codes = jnp.floor(tile * down * down * gain + 0.5).astype(jnp.int32)
    row = lax.broadcasted_iota(jnp.int32, tile.shape, 0)
    lane = lax.broadcasted_iota(jnp.int32, tile.shape, 1)
    return codes, jnp.sum(jnp.where(lane == row + first_lane, words, 0), axis=0, keepdims=True)


def packed_body(peers, source_ref, occupied_ref, summed_ref, out_ref):
    rows = summed_ref.shape[0]

    def coded(slot, first_lane):
        first = pl.multiple_of(source_ref[slot] * HS, HS)
        tile = summed_ref[:, pl.ds(first, HS)]
        return code_tile(jnp.where(occupied_ref[slot] > 0, tile, jnp.zeros_like(tile)), first_lane)

    for peer in range(peers):
        high, high_words = coded(2 * peer, SCALES)
        low, low_words = coded(2 * peer + 1, SCALES + rows)
        start = peer * (rows + 1)
        out_ref[pl.ds(start, rows), :] = (high << 16) | (low & 65535)
        out_ref[pl.ds(start + rows, 1), :] = high_words + low_words


def outgoing_body(peers, rows, packed_ref, squares_ref, out_ref):
    words, _ = words_of(jnp.sum(squares_ref[...], axis=0, keepdims=True))
    for peer in range(peers):
        start = peer * (rows + 1)
        out_ref[pl.ds(start, rows), :] = packed_ref[pl.ds(start, rows), :]
        out_ref[pl.ds(start + rows, 1), :] = packed_ref[pl.ds(start + rows, 1), :] + words


def arrived_body(peers, rows, blocks, arrived_ref, wanted_ref, owned_ref, head_ref, type_ref):
    riders = [arrived_ref[pl.ds(peer * (rows + 1) + rows, 1), :] for peer in range(peers)]
    riders = jnp.concatenate(riders, axis=0)
    mantissa = mantissa_of(riders)
    up = halves(exponent_of(riders))
    lanes = lax.broadcasted_iota(jnp.int32, riders.shape, 1)
    total = jnp.sum(jnp.where(lanes < blocks, mantissa * up * up, 0.0), axis=0, keepdims=True)
    sums = jnp.sum(wanted_ref[...] * total, axis=1, keepdims=True)
    at = lax.broadcasted_iota(jnp.int32, sums.shape, 0)
    heads = jnp.where(at < 2, 1, jnp.where(at == 2, QH, KVH))
    rms = jnp.sqrt(sums / (heads.astype(jnp.float32) * (D * HS)))
    for nth in range(2):
        head_ref[nth] = jnp.sum(jnp.where(at == nth, rms, 0.0))
    for kind in range(3):
        type_ref[kind] = jnp.sum(jnp.where(at == 2 + kind, rms, 0.0))

    step = mantissa * up * (1.0 / 32767.0)
    row = lax.broadcasted_iota(jnp.int32, (rows, HS), 0)
    lane = lax.broadcasted_iota(jnp.int32, (rows, HS), 1)

    def column(values, peer, nth):
        spread = jnp.broadcast_to(values[peer : peer + 1], (rows, HS))
        picked = jnp.where(lane == row + (SCALES + nth * rows), spread, 0.0)
        return jnp.sum(picked, axis=1, keepdims=True)

    for peer in range(peers):
        codes = arrived_ref[pl.ds(peer * (rows + 1), rows), :]
        for nth, code in enumerate((codes >> 16, (codes << 16) >> 16)):
            value = code.astype(jnp.float32) * column(step, peer, nth) * column(up, peer, nth)
            owned_ref[nth, peer] = value


def per_device(partial_grads, joined_block, head_slot):
    own_rows = partial_grads[0]
    blocks = joined_block.shape[0]
    groups = lax.axis_size(GRP)
    width = own_rows.shape[1]
    rows = own_rows.shape[0] // groups
    peers = lax.axis_size(SHARD)
    per_peer = (blocks + peers - 1) // peers
    slot_total = per_peer * peers
    first_slot = lax.axis_index(SHARD) * per_peer

    block_ids = jnp.arange(blocks, dtype=jnp.int32)
    slot_ids = jnp.arange(slot_total, dtype=jnp.int32)
    matches = (head_slot[None, :] == slot_ids[:, None]).astype(jnp.int32)
    occupied = jnp.sum(matches, axis=1)
    source = jnp.sum(matches * joined_block[None, :], axis=1)
    block_kind = (block_ids >= QH).astype(jnp.int32) + (block_ids >= QH + KVH).astype(jnp.int32)
    own = head_slot[None, :] == first_slot + jnp.arange(per_peer, dtype=jnp.int32)[:, None]
    alike = block_kind[None, :] == jnp.arange(3, dtype=jnp.int32)[:, None]
    asked = jnp.concatenate([own, alike], axis=0)
    joined = joined_block[:, None] == block_ids[None, :]
    wanted = jnp.any(asked[:, :, None] & joined[None], axis=1).astype(jnp.float32)
    wanted = jnp.pad(wanted, ((0, 8 - wanted.shape[0]), (0, HS - blocks)))

    parts = lax.all_to_all(own_rows.reshape(groups, rows, width), GRP, 0, 0, tiled=True)
    summed = jnp.sum(parts.astype(jnp.float32), axis=0)

    squares = pl.pallas_call(
        functools.partial(squares_body, blocks),
        out_shape=jax.ShapeDtypeStruct((groups, HS), jnp.float32),
        in_specs=[IN_VMEM],
        out_specs=IN_VMEM,
        compiler_params=PARAMS,
    )(summed)
    squares = lax.all_to_all(squares[:, None], GRP, split_axis=0, concat_axis=0, tiled=True)[:, 0]
    packed_shape = jax.ShapeDtypeStruct((peers * (rows + 1), HS), jnp.int32)
    packed = pl.pallas_call(
        functools.partial(packed_body, peers),
        out_shape=packed_shape,
        in_specs=[IN_SMEM, IN_SMEM, IN_VMEM],
        out_specs=IN_VMEM,
        compiler_params=PARAMS,
        cost_estimate=pl.CostEstimate(flops=4 * 10**6, bytes_accessed=2**19, transcendentals=0),
    )(source, occupied, summed)
    outgoing = pl.pallas_call(
        functools.partial(outgoing_body, peers, rows),
        out_shape=packed_shape,
        in_specs=[IN_VMEM, IN_VMEM],
        out_specs=IN_VMEM,
        compiler_params=PARAMS,
    )(packed, squares)
    arrived = lax.all_to_all(outgoing[:, None], SHARD, split_axis=0, concat_axis=0, tiled=True)
    return pl.pallas_call(
        functools.partial(arrived_body, peers, rows, blocks),
        out_shape=(
            jax.ShapeDtypeStruct((per_peer, peers, rows, HS), jnp.float32),
            jax.ShapeDtypeStruct((per_peer,), jnp.float32),
            jax.ShapeDtypeStruct((3,), jnp.float32),
        ),
        in_specs=[IN_VMEM, IN_VMEM],
        out_specs=(IN_VMEM, IN_SMEM, IN_SMEM),
        compiler_params=PARAMS,
    )(arrived[:, 0], wanted)


def solution(mesh):
    finer = Mesh(mesh.devices.reshape(8, 2, 4, 8), ("grp_0", "grp_1", "shard_0", "shard_1"))
    in_specs = (P(GRP, SHARD, None), P(), P())
    out_specs = (P(SHARD, None, GRP, None), P(SHARD), P())
    return jax.shard_map(
        per_device, mesh=finer, in_specs=in_specs, out_specs=out_specs, check_vma=False
    )
```

```python
import functools

import jax
import jax.numpy as jnp
from jax import lax
from jax.experimental import pallas as pl
from jax.experimental.pallas import tpu as pltpu
from jax.sharding import Mesh
from jax.sharding import PartitionSpec as P

D = 4096
QH = 32
KVH = 8
HS = 128
SHARD = ("shard_0", "shard_1")
GRP = ("grp_0", "grp_1")
SCALES = 64
NOISE = 1.5e-4
SPAN = 4
LOWEST = 1e-18
HIGHEST = 1e8
LIFT = 2.0**30
IN_VMEM = pl.BlockSpec(memory_space=pltpu.VMEM)
PARAMS = pltpu.CompilerParams(vmem_limit_bytes=8 * 2**20)
IN_SMEM = pl.BlockSpec(memory_space=pltpu.SMEM)


def diagonal_row(rows):
    sums = jnp.sum(rows, axis=1, keepdims=True)
    shape = rows.shape
    here = lax.broadcasted_iota(jnp.int32, shape, 0) == lax.broadcasted_iota(jnp.int32, shape, 1)
    return jnp.sum(jnp.where(here, sums, 0.0), axis=0, keepdims=True)


def squares_body(blocks, summed_ref, out_ref):
    block_rows = []
    for block in range(blocks):
        tile = summed_ref[:, pl.ds(block * HS, HS)]
        block_rows.append(jnp.sum(tile * tile, axis=0, keepdims=True))
    out_ref[...] = jnp.broadcast_to(diagonal_row(jnp.concatenate(block_rows, axis=0)), out_ref.shape)


def halves(exponent):
    return jnp.exp2(exponent * 0.5)


def words_of(values):
    exponent = jnp.floor(jnp.log2(jnp.maximum(values, 1e-37)))
    down = halves(-exponent)
    mantissa = jnp.floor(values * down * down * 2.0**18).astype(jnp.int32) + 1
    return jnp.where(values > 0.0, mantissa * 1024 + exponent.astype(jnp.int32) + 512, 0), exponent


def mantissa_of(words):
    return (words >> 10).astype(jnp.float32) * 2.0**-18


def exponent_of(words):
    return ((words & 1023) - 512).astype(jnp.float32)


def count_body(peers, rows, blocks, arrived_ref, out_ref):
    riders = [arrived_ref[pl.ds(peer * (rows + 1) + rows, 1), :] for peer in range(peers)]
    riders = jnp.concatenate(riders, axis=0)
    lane = lax.broadcasted_iota(jnp.int32, riders.shape, 1)
    out_ref[0] = jnp.sum(jnp.where((lane == blocks) & (riders != 0), 1.0, 0.0))


def value_of(words):
    up = halves(exponent_of(words))
    return mantissa_of(words) * up * up


def code_tile(tile, first_lane):
    most = jnp.max(jnp.abs(tile), axis=1, keepdims=True)
    words, exponent = words_of(most)
    down = halves(-exponent)
    gain = 32767.0 / jnp.where(words > 0, mantissa_of(words), 1.0)
    codes = jnp.floor(tile * down * down * gain + 0.5).astype(jnp.int32)
    row = lax.broadcasted_iota(jnp.int32, tile.shape, 0)
    lane = lax.broadcasted_iota(jnp.int32, tile.shape, 1)
    return codes, jnp.sum(jnp.where(lane == row + first_lane, words, 0), axis=0, keepdims=True)


def packed_body(peers, source_ref, occupied_ref, summed_ref, out_ref):
    rows = summed_ref.shape[0]

    def coded(slot, first_lane):
        first = pl.multiple_of(source_ref[slot] * HS, HS)
        tile = summed_ref[:, pl.ds(first, HS)]
        return code_tile(jnp.where(occupied_ref[slot] > 0, tile, jnp.zeros_like(tile)), first_lane)

    for peer in range(peers):
        high, high_words = coded(2 * peer, SCALES)
        low, low_words = coded(2 * peer + 1, SCALES + rows)
        start = peer * (rows + 1)
        out_ref[pl.ds(start, rows), :] = (high << 16) | (low & 65535)
        out_ref[pl.ds(start + rows, 1), :] = high_words + low_words


def outgoing_body(peers, rows, packed_ref, squares_ref, out_ref):
    words, _ = words_of(jnp.sum(squares_ref[...], axis=0, keepdims=True))
    for peer in range(peers):
        start = peer * (rows + 1)
        out_ref[pl.ds(start, rows), :] = packed_ref[pl.ds(start, rows), :]
        out_ref[pl.ds(start + rows, 1), :] = packed_ref[pl.ds(start + rows, 1), :] + words


def arrived_body(peers, rows, blocks, arrived_ref, wanted_ref, owned_ref, head_ref, type_ref):
    riders = [arrived_ref[pl.ds(peer * (rows + 1) + rows, 1), :] for peer in range(peers)]
    riders = jnp.concatenate(riders, axis=0)
    mantissa = mantissa_of(riders)
    up = halves(exponent_of(riders))
    lanes = lax.broadcasted_iota(jnp.int32, riders.shape, 1)
    total = jnp.sum(jnp.where(lanes < blocks, mantissa * up * up, 0.0), axis=0, keepdims=True)
    sums = jnp.sum(wanted_ref[...] * total, axis=1, keepdims=True)
    at = lax.broadcasted_iota(jnp.int32, sums.shape, 0)
    heads = jnp.where(at < 2, 1, jnp.where(at == 2, QH, KVH))
    rms = jnp.sqrt(sums / (heads.astype(jnp.float32) * (D * HS)))
    for nth in range(2):
        head_ref[nth] = jnp.sum(jnp.where(at == nth, rms, 0.0))
    for kind in range(3):
        type_ref[kind] = jnp.sum(jnp.where(at == 2 + kind, rms, 0.0))

    step = mantissa * up * (1.0 / 32767.0)
    row = lax.broadcasted_iota(jnp.int32, (rows, HS), 0)
    lane = lax.broadcasted_iota(jnp.int32, (rows, HS), 1)

    def column(values, peer, nth):
        spread = jnp.broadcast_to(values[peer : peer + 1], (rows, HS))
        picked = jnp.where(lane == row + (SCALES + nth * rows), spread, 0.0)
        return jnp.sum(picked, axis=1, keepdims=True)

    for peer in range(peers):
        codes = arrived_ref[pl.ds(peer * (rows + 1), rows), :]
        for nth, code in enumerate((codes >> 16, (codes << 16) >> 16)):
            value = code.astype(jnp.float32) * column(step, peer, nth) * column(up, peer, nth)
            owned_ref[nth, peer] = value


def pair_body(sums_ref, out_ref):
    chunks, rows, width = sums_ref.shape
    half = width // 2
    lane = lax.broadcasted_iota(jnp.int32, (rows, HS), 1)

    def chunk_step(chunk, _):
        most = jnp.zeros((rows, HS), jnp.float32)
        for span in range(width // (SPAN * HS)):
            tiles = [sums_ref[chunk, :, pl.ds((SPAN * span + nth) * HS, HS)] for nth in range(SPAN)]
            peak = functools.reduce(jnp.maximum, [jnp.abs(tile) for tile in tiles])
            most = jnp.where(lane == span, jnp.max(peak, axis=1, keepdims=True), most)
        words, _ = words_of(jnp.minimum(most, 2.0 * HIGHEST))
        out_ref[chunk, :, pl.ds(half, HS)] = words
        gain = jnp.where(words > 0, 32767.0 / jnp.maximum(value_of(words), LOWEST * 0.5), 0.0)
        spans = width // (SPAN * HS)
        gains = [jnp.broadcast_to(gain[:, span : span + 1], (rows, HS)) for span in range(spans)]
        for block in range(half // HS):
            codes = []
            for place in (block, block + half // HS):
                tile = sums_ref[chunk, :, pl.ds(place * HS, HS)]
                codes.append(jnp.floor(tile * gains[place // SPAN] + 0.5).astype(jnp.int32))
            out_ref[chunk, :, pl.ds(block * HS, HS)] = (codes[0] << 16) | (codes[1] & 65535)
        return 0

    lax.fori_loop(0, chunks, chunk_step, 0)


def gathered_body(words_ref, summed_ref, out_ref):
    chunks, rows, width = words_ref.shape
    half = width - HS
    blocks = 2 * half // HS
    scales = [value_of(words_ref[chunk, :, pl.ds(half, HS)]) for chunk in range(chunks)]
    lane = lax.broadcasted_iota(jnp.int32, (rows, HS), 1)
    odd = jnp.zeros((rows, HS), jnp.float32)
    noise = jnp.zeros((rows, HS), jnp.float32)
    for scale in scales:
        strange = (scale > HIGHEST) | ((scale > 0.0) & (scale < LOWEST))
        odd = jnp.where(strange, 1.0, odd)
        step = jnp.minimum(scale, HIGHEST) * (LIFT / 32767.0)
        noise = noise + step * step * (HS / 12.0)
    scales = [scale * (1.0 / 32767.0) for scale in scales]
    noise = jnp.sum(noise, axis=0, keepdims=True)
    noises = [jnp.where(lane[:1] // SPAN == span, noise[:, span : span + 1], 0.0) for span in range(blocks // SPAN)]
    noise = functools.reduce(jnp.add, noises)
    block_rows = [None] * blocks
    for block in range(half // HS):
        if block % SPAN == 0:
            firsts = (block // SPAN, (block + half // HS) // SPAN)
            steps = [
                [jnp.broadcast_to(scale[:, span : span + 1], (rows, HS)) for span in firsts] for scale in scales
            ]
        totals = [jnp.zeros((rows, HS), jnp.float32)] * 2
        for chunk in range(chunks):
            both = words_ref[chunk, :, pl.ds(block * HS, HS)]
            for nth, code in enumerate((both >> 16, (both << 16) >> 16)):
                totals[nth] = totals[nth] + code.astype(jnp.float32) * steps[chunk][nth]
        for nth, total in enumerate(totals):
            place = block + nth * (half // HS)
            summed_ref[:, pl.ds(place * HS, HS)] = total
            block_rows[place] = jnp.sum(total * total, axis=0, keepdims=True)
    squares = diagonal_row(jnp.concatenate(block_rows, axis=0))
    odd = jnp.sum(odd, axis=0, keepdims=True)
    bad = (noise > (LIFT * NOISE) ** 2 * squares) & (lane[:1] < blocks)
    count = jnp.sum(jnp.where(bad, 1.0, 0.0) + odd, axis=1, keepdims=True)
    out_ref[...] = jnp.broadcast_to(jnp.where(lane[:1] == blocks, count, squares), out_ref.shape)


def kernel(body, out_shape, in_specs, out_specs, flops=None):
    cost = flops and pl.CostEstimate(flops=flops, bytes_accessed=2**19, transcendentals=0)
    return pl.pallas_call(
        body,
        out_shape=out_shape,
        in_specs=in_specs,
        out_specs=out_specs,
        compiler_params=PARAMS,
        cost_estimate=cost,
    )


def to_groups(squares):
    return lax.all_to_all(squares[:, None], GRP, split_axis=0, concat_axis=0, tiled=True)[:, 0]


def exact_sums(own, blocks):
    parts = lax.all_to_all(own, GRP, 0, 0, tiled=True)
    summed = jnp.sum(parts.astype(jnp.float32), axis=0)
    shape = jax.ShapeDtypeStruct((own.shape[0], HS), jnp.float32)
    squares = kernel(functools.partial(squares_body, blocks), shape, [IN_VMEM], IN_VMEM)(summed)
    return summed, squares


def coded_sums(own):
    groups, rows, width = own.shape
    core = lax.axis_index("grp_1")
    pairs = own.reshape(groups // 2, 2, rows, width)
    give = lax.dynamic_index_in_dim(pairs, 1 - core, 1, keepdims=False)
    keep = lax.dynamic_index_in_dim(pairs, core, 1, keepdims=False)
    got = lax.ppermute(give, "grp_1", [(0, 1), (1, 0)])
    sums = keep.astype(jnp.float32) + got.astype(jnp.float32)
    shape = jax.ShapeDtypeStruct((groups // 2, rows, width // 2 + HS), jnp.int32)
    words = kernel(pair_body, shape, [IN_VMEM], IN_VMEM)(sums)
    words = lax.all_to_all(words, "grp_0", 0, 0, tiled=True)
    shapes = (
        jax.ShapeDtypeStruct((rows, width), jnp.float32),
        jax.ShapeDtypeStruct((groups, HS), jnp.float32),
    )
    return kernel(gathered_body, shapes, [IN_VMEM], (IN_VMEM, IN_VMEM))(words)


def shard_exchange(source, occupied, summed, squares):
    rows = summed.shape[0]
    peers = lax.axis_size(SHARD)
    shape = jax.ShapeDtypeStruct((peers * (rows + 1), HS), jnp.int32)
    specs = [IN_SMEM, IN_SMEM, IN_VMEM]
    squares = to_groups(squares)
    packed = kernel(functools.partial(packed_body, peers), shape, specs, IN_VMEM, 4 * 10**6)(source, occupied, summed)
    body = functools.partial(outgoing_body, peers, rows)
    outgoing = kernel(body, shape, [IN_VMEM, IN_VMEM], IN_VMEM)(packed, squares)
    return lax.all_to_all(outgoing[:, None], SHARD, split_axis=0, concat_axis=0, tiled=True)[:, 0]


def unpacked(arrived, wanted, *, blocks, rows, per_peer):
    peers = arrived.shape[0] // (rows + 1)
    shapes = (
        jax.ShapeDtypeStruct((per_peer, peers, rows, HS), jnp.float32),
        jax.ShapeDtypeStruct((per_peer,), jnp.float32),
        jax.ShapeDtypeStruct((3,), jnp.float32),
    )
    body = functools.partial(arrived_body, peers, rows, blocks)
    return kernel(body, shapes, [IN_VMEM, IN_VMEM], (IN_VMEM, IN_SMEM, IN_SMEM))(arrived, wanted)


def per_device(partial_grads, joined_block, head_slot):
    own_rows = partial_grads[0]
    blocks = joined_block.shape[0]
    groups = lax.axis_size(GRP)
    width = own_rows.shape[1]
    rows = own_rows.shape[0] // groups
    peers = lax.axis_size(SHARD)
    per_peer = (blocks + peers - 1) // peers
    slot_total = per_peer * peers
    first_slot = lax.axis_index(SHARD) * per_peer

    block_ids = jnp.arange(blocks, dtype=jnp.int32)
    slot_ids = jnp.arange(slot_total, dtype=jnp.int32)
    matches = (head_slot[None, :] == slot_ids[:, None]).astype(jnp.int32)
    occupied = jnp.sum(matches, axis=1)
    source = jnp.sum(matches * joined_block[None, :], axis=1)
    block_kind = (block_ids >= QH).astype(jnp.int32) + (block_ids >= QH + KVH).astype(jnp.int32)
    own = head_slot[None, :] == first_slot + jnp.arange(per_peer, dtype=jnp.int32)[:, None]
    alike = block_kind[None, :] == jnp.arange(3, dtype=jnp.int32)[:, None]
    asked = jnp.concatenate([own, alike], axis=0)
    joined = joined_block[:, None] == block_ids[None, :]
    wanted = jnp.any(asked[:, :, None] & joined[None], axis=1).astype(jnp.float32)
    wanted = jnp.pad(wanted, ((0, 8 - wanted.shape[0]), (0, HS - blocks)))

    finish = functools.partial(shard_exchange, source, occupied)
    arrived = finish(*coded_sums(own_rows.reshape(groups, rows, width)))
    body = functools.partial(count_body, peers, rows, blocks)
    failed = kernel(body, jax.ShapeDtypeStruct((1,), jnp.float32), [IN_VMEM], IN_SMEM)(arrived)
    unpack = functools.partial(unpacked, blocks=blocks, rows=rows, per_peer=per_peer)

    def exactly(own, mine, weights):
        return unpack(finish(*exact_sums(own, blocks)), weights)

    def as_coded(own, mine, weights):
        return unpack(mine, weights)

    return lax.cond(failed[0] > 0.0, exactly, as_coded, own_rows.reshape(groups, rows, width), arrived, wanted)


def solution(mesh):
    finer = Mesh(mesh.devices.reshape(8, 2, 4, 8), ("grp_0", "grp_1", "shard_0", "shard_1"))
    in_specs = (P(GRP, SHARD, None), P(), P())
    out_specs = (P(SHARD, None, GRP, None), P(SHARD), P())
    return jax.shard_map(
        per_device, mesh=finer, in_specs=in_specs, out_specs=out_specs, check_vma=False
    )
```

```python
import functools

import jax
import jax.numpy as jnp
from jax import lax
from jax.experimental import pallas as pl
from jax.experimental.pallas import tpu as pltpu
from jax.sharding import Mesh
from jax.sharding import PartitionSpec as P

D = 4096
QH = 32
KVH = 8
HS = 128
SHARD = ("shard_0", "shard_1")
GRP = ("grp_0", "grp_1")
SCALES = 64
NOISE = 1.5e-4
SPAN = 4
LOWEST = 1e-18
HIGHEST = 1e8
LIFT = 2.0**30
IN_VMEM = pl.BlockSpec(memory_space=pltpu.VMEM)
PARAMS = pltpu.CompilerParams(vmem_limit_bytes=8 * 2**20)
IN_SMEM = pl.BlockSpec(memory_space=pltpu.SMEM)


def diagonal_row(rows):
    sums = jnp.sum(rows, axis=1, keepdims=True)
    shape = rows.shape
    here = lax.broadcasted_iota(jnp.int32, shape, 0) == lax.broadcasted_iota(jnp.int32, shape, 1)
    return jnp.sum(jnp.where(here, sums, 0.0), axis=0, keepdims=True)


def squares_body(blocks, summed_ref, out_ref):
    block_rows = []
    for block in range(blocks):
        tile = summed_ref[:, pl.ds(block * HS, HS)]
        block_rows.append(jnp.sum(tile * tile, axis=0, keepdims=True))
    out_ref[...] = jnp.broadcast_to(diagonal_row(jnp.concatenate(block_rows, axis=0)), out_ref.shape)


def halves(exponent):
    return jnp.exp2(exponent * 0.5)


def words_of(values):
    exponent = jnp.floor(jnp.log2(jnp.maximum(values, 1e-37)))
    down = halves(-exponent)
    mantissa = jnp.floor(values * down * down * 2.0**18).astype(jnp.int32) + 1
    return jnp.where(values > 0.0, mantissa * 1024 + exponent.astype(jnp.int32) + 512, 0), exponent


def mantissa_of(words):
    return (words >> 10).astype(jnp.float32) * 2.0**-18


def exponent_of(words):
    return ((words & 1023) - 512).astype(jnp.float32)


def value_of(words):
    up = halves(exponent_of(words))
    return mantissa_of(words) * up * up


def code_tile(tile, first_lane):
    most = jnp.max(jnp.abs(tile), axis=1, keepdims=True)
    words, exponent = words_of(most)
    down = halves(-exponent)
    gain = 32767.0 / jnp.where(words > 0, mantissa_of(words), 1.0)
    codes = jnp.floor(tile * down * down * gain + 0.5).astype(jnp.int32)
    row = lax.broadcasted_iota(jnp.int32, tile.shape, 0)
    lane = lax.broadcasted_iota(jnp.int32, tile.shape, 1)
    return codes, jnp.sum(jnp.where(lane == row + first_lane, words, 0), axis=0, keepdims=True)


def packed_body(peers, source_ref, occupied_ref, summed_ref, out_ref):
    rows = summed_ref.shape[0]

    def coded(slot, first_lane):
        first = pl.multiple_of(source_ref[slot] * HS, HS)
        tile = summed_ref[:, pl.ds(first, HS)]
        return code_tile(jnp.where(occupied_ref[slot] > 0, tile, jnp.zeros_like(tile)), first_lane)

    for peer in range(peers):
        high, high_words = coded(2 * peer, SCALES)
        low, low_words = coded(2 * peer + 1, SCALES + rows)
        start = peer * (rows + 1)
        out_ref[pl.ds(start, rows), :] = (high << 16) | (low & 65535)
        out_ref[pl.ds(start + rows, 1), :] = high_words + low_words


def outgoing_body(peers, rows, packed_ref, squares_ref, out_ref):
    words, _ = words_of(jnp.sum(squares_ref[...], axis=0, keepdims=True))
    for peer in range(peers):
        start = peer * (rows + 1)
        out_ref[pl.ds(start, rows), :] = packed_ref[pl.ds(start, rows), :]
        out_ref[pl.ds(start + rows, 1), :] = packed_ref[pl.ds(start + rows, 1), :] + words


def arrived_body(peers, rows, blocks, arrived_ref, wanted_ref, owned_ref, head_ref, type_ref, failed_ref):
    riders = [arrived_ref[pl.ds(peer * (rows + 1) + rows, 1), :] for peer in range(peers)]
    riders = jnp.concatenate(riders, axis=0)
    mantissa = mantissa_of(riders)
    up = halves(exponent_of(riders))
    lanes = lax.broadcasted_iota(jnp.int32, riders.shape, 1)
    failed_ref[0] = jnp.sum(jnp.where((lanes == blocks) & (riders != 0), 1.0, 0.0))
    total = jnp.sum(jnp.where(lanes < blocks, mantissa * up * up, 0.0), axis=0, keepdims=True)
    sums = jnp.sum(wanted_ref[...] * total, axis=1, keepdims=True)
    at = lax.broadcasted_iota(jnp.int32, sums.shape, 0)
    heads = jnp.where(at < 2, 1, jnp.where(at == 2, QH, KVH))
    rms = jnp.sqrt(sums / (heads.astype(jnp.float32) * (D * HS)))
    for nth in range(2):
        head_ref[nth] = jnp.sum(jnp.where(at == nth, rms, 0.0))
    for kind in range(3):
        type_ref[kind] = jnp.sum(jnp.where(at == 2 + kind, rms, 0.0))

    step = mantissa * up * (1.0 / 32767.0)
    row = lax.broadcasted_iota(jnp.int32, (rows, HS), 0)
    lane = lax.broadcasted_iota(jnp.int32, (rows, HS), 1)

    def column(values, peer, nth):
        spread = jnp.broadcast_to(values[peer : peer + 1], (rows, HS))
        picked = jnp.where(lane == row + (SCALES + nth * rows), spread, 0.0)
        return jnp.sum(picked, axis=1, keepdims=True)

    for peer in range(peers):
        codes = arrived_ref[pl.ds(peer * (rows + 1), rows), :]
        for nth, code in enumerate((codes >> 16, (codes << 16) >> 16)):
            value = code.astype(jnp.float32) * column(step, peer, nth) * column(up, peer, nth)
            owned_ref[nth, peer] = value


def pair_body(sums_ref, out_ref):
    chunks, rows, width = sums_ref.shape
    half = width // 2
    lane = lax.broadcasted_iota(jnp.int32, (rows, HS), 1)

    def tile(chunk, place):
        return sums_ref[chunk, :, pl.ds(place * HS, HS)]

    gains = []
    for chunk in range(chunks):
        most = jnp.zeros((rows, HS), jnp.float32)
        for span in range(width // (SPAN * HS)):
            peaks = [jnp.abs(tile(chunk, SPAN * span + nth)) for nth in range(SPAN)]
            peak = jnp.max(functools.reduce(jnp.maximum, peaks), axis=1, keepdims=True)
            most = jnp.where(lane == span, peak, most)
        words, _ = words_of(jnp.minimum(most, 2.0 * HIGHEST))
        out_ref[chunk, :, pl.ds(half, HS)] = words
        gains.append(jnp.where(words > 0, 32767.0 / jnp.maximum(value_of(words), LOWEST * 0.5), 0.0))
    for chunk in range(chunks):
        for block in range(half // HS):
            codes = []
            for place in (block, block + half // HS):
                span = place // SPAN
                value = tile(chunk, place) * gains[chunk][:, span : span + 1]
                codes.append(jnp.floor(value + 0.5).astype(jnp.int32))
            out_ref[chunk, :, pl.ds(block * HS, HS)] = (codes[0] << 16) | (codes[1] & 65535)


def gathered_body(words_ref, summed_ref, out_ref):
    chunks, rows, width = words_ref.shape
    half = width - HS
    blocks = 2 * half // HS
    scales = [value_of(words_ref[chunk, :, pl.ds(half, HS)]) for chunk in range(chunks)]
    lane = lax.broadcasted_iota(jnp.int32, (rows, HS), 1)
    odd = jnp.zeros((rows, HS), jnp.float32)
    noise = jnp.zeros((rows, HS), jnp.float32)
    for scale in scales:
        strange = (scale > HIGHEST) | ((scale > 0.0) & (scale < LOWEST))
        odd = jnp.where(strange, 1.0, odd)
        step = jnp.minimum(scale, HIGHEST) * (LIFT / 32767.0)
        noise = noise + step * step * (HS / 12.0)
    scales = [scale * (1.0 / 32767.0) for scale in scales]
    noise = jnp.sum(noise, axis=0, keepdims=True)
    noises = [jnp.where(lane[:1] // SPAN == span, noise[:, span : span + 1], 0.0) for span in range(blocks // SPAN)]
    noise = functools.reduce(jnp.add, noises)
    block_rows = [None] * blocks
    for block in range(half // HS):
        if block % SPAN == 0:
            firsts = (block // SPAN, (block + half // HS) // SPAN)
            steps = [
                [jnp.broadcast_to(scale[:, span : span + 1], (rows, HS)) for span in firsts] for scale in scales
            ]
        totals = [jnp.zeros((rows, HS), jnp.float32)] * 2
        for chunk in range(chunks):
            both = words_ref[chunk, :, pl.ds(block * HS, HS)]
            for nth, code in enumerate((both >> 16, (both << 16) >> 16)):
                totals[nth] = totals[nth] + code.astype(jnp.float32) * steps[chunk][nth]
        for nth, total in enumerate(totals):
            place = block + nth * (half // HS)
            summed_ref[:, pl.ds(place * HS, HS)] = total
            block_rows[place] = jnp.sum(total * total, axis=0, keepdims=True)
    squares = diagonal_row(jnp.concatenate(block_rows, axis=0))
    odd = jnp.sum(odd, axis=0, keepdims=True)
    bad = (noise > (LIFT * NOISE) ** 2 * squares) & (lane[:1] < blocks)
    count = jnp.sum(jnp.where(bad, 1.0, 0.0) + odd, axis=1, keepdims=True)
    out_ref[...] = jnp.broadcast_to(jnp.where(lane[:1] == blocks, count, squares), out_ref.shape)


def kernel(body, out_shape, in_specs, out_specs, flops=None):
    cost = flops and pl.CostEstimate(flops=flops, bytes_accessed=2**19, transcendentals=0)
    return pl.pallas_call(
        body,
        out_shape=out_shape,
        in_specs=in_specs,
        out_specs=out_specs,
        compiler_params=PARAMS,
        cost_estimate=cost,
    )


def to_groups(squares):
    return lax.all_to_all(squares[:, None], GRP, split_axis=0, concat_axis=0, tiled=True)[:, 0]


def exact_sums(own, blocks):
    parts = lax.all_to_all(own, GRP, 0, 0, tiled=True)
    summed = jnp.sum(parts.astype(jnp.float32), axis=0)
    shape = jax.ShapeDtypeStruct((own.shape[0], HS), jnp.float32)
    squares = kernel(functools.partial(squares_body, blocks), shape, [IN_VMEM], IN_VMEM)(summed)
    return summed, squares


def coded_sums(own):
    groups, rows, width = own.shape
    core = lax.axis_index("grp_1")
    pairs = own.reshape(groups // 2, 2, rows, width)
    give = lax.dynamic_index_in_dim(pairs, 1 - core, 1, keepdims=False)
    keep = lax.dynamic_index_in_dim(pairs, core, 1, keepdims=False)
    got = lax.ppermute(give, "grp_1", [(0, 1), (1, 0)])
    sums = keep.astype(jnp.float32) + got.astype(jnp.float32)
    shape = jax.ShapeDtypeStruct((groups // 2, rows, width // 2 + HS), jnp.int32)
    words = kernel(pair_body, shape, [IN_VMEM], IN_VMEM)(sums)
    words = lax.all_to_all(words, "grp_0", 0, 0, tiled=True)
    shapes = (
        jax.ShapeDtypeStruct((rows, width), jnp.float32),
        jax.ShapeDtypeStruct((groups, HS), jnp.float32),
    )
    return kernel(gathered_body, shapes, [IN_VMEM], (IN_VMEM, IN_VMEM))(words)


def shard_exchange(source, occupied, summed, squares):
    rows = summed.shape[0]
    peers = lax.axis_size(SHARD)
    shape = jax.ShapeDtypeStruct((peers * (rows + 1), HS), jnp.int32)
    specs = [IN_SMEM, IN_SMEM, IN_VMEM]
    squares = to_groups(squares)
    packed = kernel(functools.partial(packed_body, peers), shape, specs, IN_VMEM, 4 * 10**6)(source, occupied, summed)
    body = functools.partial(outgoing_body, peers, rows)
    outgoing = kernel(body, shape, [IN_VMEM, IN_VMEM], IN_VMEM)(packed, squares)
    return lax.all_to_all(outgoing[:, None], SHARD, split_axis=0, concat_axis=0, tiled=True)[:, 0]


def unpacked(arrived, wanted, *, blocks, rows, per_peer):
    peers = arrived.shape[0] // (rows + 1)
    shapes = (
        jax.ShapeDtypeStruct((per_peer, peers, rows, HS), jnp.float32),
        jax.ShapeDtypeStruct((per_peer,), jnp.float32),
        jax.ShapeDtypeStruct((3,), jnp.float32),
        jax.ShapeDtypeStruct((1,), jnp.float32),
    )
    body = functools.partial(arrived_body, peers, rows, blocks)
    specs = (IN_VMEM, IN_SMEM, IN_SMEM, IN_SMEM)
    return kernel(body, shapes, [IN_VMEM, IN_VMEM], specs)(arrived, wanted)


def per_device(partial_grads, joined_block, head_slot):
    own_rows = partial_grads[0]
    blocks = joined_block.shape[0]
    groups = lax.axis_size(GRP)
    width = own_rows.shape[1]
    rows = own_rows.shape[0] // groups
    peers = lax.axis_size(SHARD)
    per_peer = (blocks + peers - 1) // peers
    slot_total = per_peer * peers
    first_slot = lax.axis_index(SHARD) * per_peer

    block_ids = jnp.arange(blocks, dtype=jnp.int32)
    slot_ids = jnp.arange(slot_total, dtype=jnp.int32)
    matches = (head_slot[None, :] == slot_ids[:, None]).astype(jnp.int32)
    occupied = jnp.sum(matches, axis=1)
    source = jnp.sum(matches * joined_block[None, :], axis=1)
    block_kind = (block_ids >= QH).astype(jnp.int32) + (block_ids >= QH + KVH).astype(jnp.int32)
    own = head_slot[None, :] == first_slot + jnp.arange(per_peer, dtype=jnp.int32)[:, None]
    alike = block_kind[None, :] == jnp.arange(3, dtype=jnp.int32)[:, None]
    asked = jnp.concatenate([own, alike], axis=0)
    joined = joined_block[:, None] == block_ids[None, :]
    wanted = jnp.any(asked[:, :, None] & joined[None], axis=1).astype(jnp.float32)
    wanted = jnp.pad(wanted, ((0, 8 - wanted.shape[0]), (0, HS - blocks)))

    finish = functools.partial(shard_exchange, source, occupied)
    arrived = finish(*coded_sums(own_rows.reshape(groups, rows, width)))
    unpack = functools.partial(unpacked, wanted=wanted, blocks=blocks, rows=rows, per_peer=per_peer)

    def exactly(state):
        own = jnp.where(state[3][0] > 0.0, own_rows, jnp.zeros_like(own_rows))
        return unpack(finish(*exact_sums(own.reshape(groups, rows, width), blocks)))

    results = lax.while_loop(lambda state: state[3][0] > 0.0, exactly, unpack(arrived))
    return results[:3]


def solution(mesh):
    finer = Mesh(mesh.devices.reshape(8, 2, 4, 8), ("grp_0", "grp_1", "shard_0", "shard_1"))
    in_specs = (P(GRP, SHARD, None), P(), P())
    out_specs = (P(SHARD, None, GRP, None), P(SHARD), P())
    return jax.shard_map(
        per_device, mesh=finer, in_specs=in_specs, out_specs=out_specs, check_vma=False
    )
```

```python
import functools

import jax
import jax.numpy as jnp
from jax import lax
from jax.experimental import pallas as pl
from jax.experimental.pallas import tpu as pltpu
from jax.sharding import Mesh
from jax.sharding import PartitionSpec as P

D = 4096
QH = 32
KVH = 8
HS = 128
SHARD = ("shard_0", "shard_1")
GRP = ("grp_0", "grp_1")
SCALES = 64
NOISE = 1e-4
SPAN = 2
LOWEST = 1e-18
HIGHEST = 1e8
LIFT = 2.0**30
IN_VMEM = pl.BlockSpec(memory_space=pltpu.VMEM)
PARAMS = pltpu.CompilerParams(vmem_limit_bytes=8 * 2**20)
IN_SMEM = pl.BlockSpec(memory_space=pltpu.SMEM)


def diagonal_row(rows):
    sums = jnp.sum(rows, axis=1, keepdims=True)
    shape = rows.shape
    here = lax.broadcasted_iota(jnp.int32, shape, 0) == lax.broadcasted_iota(jnp.int32, shape, 1)
    return jnp.sum(jnp.where(here, sums, 0.0), axis=0, keepdims=True)


def squares_body(blocks, summed_ref, out_ref):
    block_rows = []
    for block in range(blocks):
        tile = summed_ref[:, pl.ds(block * HS, HS)]
        block_rows.append(jnp.sum(tile * tile, axis=0, keepdims=True))
    out_ref[...] = jnp.broadcast_to(diagonal_row(jnp.concatenate(block_rows, axis=0)), out_ref.shape)


def halves(exponent):
    return jnp.exp2(exponent * 0.5)


def words_of(values):
    exponent = jnp.floor(jnp.log2(jnp.maximum(values, 1e-37)))
    down = halves(-exponent)
    mantissa = jnp.floor(values * down * down * 2.0**18).astype(jnp.int32) + 1
    return jnp.where(values > 0.0, mantissa * 1024 + exponent.astype(jnp.int32) + 512, 0), exponent


def mantissa_of(words):
    return (words >> 10).astype(jnp.float32) * 2.0**-18


def exponent_of(words):
    return ((words & 1023) - 512).astype(jnp.float32)


def value_of(words):
    up = halves(exponent_of(words))
    return mantissa_of(words) * up * up


def code_tile(tile, first_lane):
    most = jnp.max(jnp.abs(tile), axis=1, keepdims=True)
    words, exponent = words_of(most)
    down = halves(-exponent)
    gain = 32767.0 / jnp.where(words > 0, mantissa_of(words), 1.0)
    codes = jnp.floor(tile * down * down * gain + 0.5).astype(jnp.int32)
    row = lax.broadcasted_iota(jnp.int32, tile.shape, 0)
    lane = lax.broadcasted_iota(jnp.int32, tile.shape, 1)
    return codes, jnp.sum(jnp.where(lane == row + first_lane, words, 0), axis=0, keepdims=True)


def packed_body(peers, source_ref, occupied_ref, summed_ref, out_ref):
    rows = summed_ref.shape[0]

    def coded(slot, first_lane):
        first = pl.multiple_of(source_ref[slot] * HS, HS)
        tile = summed_ref[:, pl.ds(first, HS)]
        return code_tile(jnp.where(occupied_ref[slot] > 0, tile, jnp.zeros_like(tile)), first_lane)

    for peer in range(peers):
        high, high_words = coded(2 * peer, SCALES)
        low, low_words = coded(2 * peer + 1, SCALES + rows)
        start = peer * (rows + 1)
        out_ref[pl.ds(start, rows), :] = (high << 16) | (low & 65535)
        out_ref[pl.ds(start + rows, 1), :] = high_words + low_words


def outgoing_body(peers, rows, packed_ref, squares_ref, out_ref):
    words, _ = words_of(jnp.sum(squares_ref[...], axis=0, keepdims=True))
    for peer in range(peers):
        start = peer * (rows + 1)
        out_ref[pl.ds(start, rows), :] = packed_ref[pl.ds(start, rows), :]
        out_ref[pl.ds(start + rows, 1), :] = packed_ref[pl.ds(start + rows, 1), :] + words


def arrived_body(peers, rows, blocks, arrived_ref, wanted_ref, owned_ref, head_ref, type_ref, failed_ref):
    riders = [arrived_ref[pl.ds(peer * (rows + 1) + rows, 1), :] for peer in range(peers)]
    riders = jnp.concatenate(riders, axis=0)
    mantissa = mantissa_of(riders)
    up = halves(exponent_of(riders))
    lanes = lax.broadcasted_iota(jnp.int32, riders.shape, 1)
    failed_ref[0] = jnp.sum(jnp.where((lanes == blocks) & (riders != 0), 1.0, 0.0))
    total = jnp.sum(jnp.where(lanes < blocks, mantissa * up * up, 0.0), axis=0, keepdims=True)
    sums = jnp.sum(wanted_ref[...] * total, axis=1, keepdims=True)
    at = lax.broadcasted_iota(jnp.int32, sums.shape, 0)
    heads = jnp.where(at < 2, 1, jnp.where(at == 2, QH, KVH))
    rms = jnp.sqrt(sums / (heads.astype(jnp.float32) * (D * HS)))
    for nth in range(2):
        head_ref[nth] = jnp.sum(jnp.where(at == nth, rms, 0.0))
    for kind in range(3):
        type_ref[kind] = jnp.sum(jnp.where(at == 2 + kind, rms, 0.0))

    step = mantissa * up * (1.0 / 32767.0)
    row = lax.broadcasted_iota(jnp.int32, (rows, HS), 0)
    lane = lax.broadcasted_iota(jnp.int32, (rows, HS), 1)

    def column(values, peer, nth):
        spread = jnp.broadcast_to(values[peer : peer + 1], (rows, HS))
        picked = jnp.where(lane == row + (SCALES + nth * rows), spread, 0.0)
        return jnp.sum(picked, axis=1, keepdims=True)

    for peer in range(peers):
        codes = arrived_ref[pl.ds(peer * (rows + 1), rows), :]
        for nth, code in enumerate((codes >> 16, (codes << 16) >> 16)):
            value = code.astype(jnp.float32) * column(step, peer, nth) * column(up, peer, nth)
            owned_ref[nth, peer] = value


def pair_body(sums_ref, out_ref):
    chunks, rows, width = sums_ref.shape
    half = width // 2
    lane = lax.broadcasted_iota(jnp.int32, (rows, HS), 1)

    def tile(chunk, place):
        return sums_ref[chunk, :, pl.ds(place * HS, HS)]

    gains = []
    for chunk in range(chunks):
        most = jnp.zeros((rows, HS), jnp.float32)
        for span in range(width // (SPAN * HS)):
            peaks = [jnp.abs(tile(chunk, SPAN * span + nth)) for nth in range(SPAN)]
            peak = jnp.max(functools.reduce(jnp.maximum, peaks), axis=1, keepdims=True)
            most = jnp.where(lane == span, peak, most)
        words, _ = words_of(jnp.minimum(most, 2.0 * HIGHEST))
        out_ref[chunk, :, pl.ds(half, HS)] = words
        gains.append(jnp.where(words > 0, 32767.0 / jnp.maximum(value_of(words), LOWEST * 0.5), 0.0))
    for chunk in range(chunks):
        for block in range(half // HS):
            codes = []
            for place in (block, block + half // HS):
                span = place // SPAN
                value = tile(chunk, place) * gains[chunk][:, span : span + 1]
                codes.append(jnp.floor(value + 0.5).astype(jnp.int32))
            out_ref[chunk, :, pl.ds(block * HS, HS)] = (codes[0] << 16) | (codes[1] & 65535)


def gathered_body(words_ref, summed_ref, out_ref):
    chunks, rows, width = words_ref.shape
    half = width - HS
    blocks = 2 * half // HS
    scales = [value_of(words_ref[chunk, :, pl.ds(half, HS)]) for chunk in range(chunks)]
    lane = lax.broadcasted_iota(jnp.int32, (rows, HS), 1)
    odd = jnp.zeros((rows, HS), jnp.float32)
    noise = jnp.zeros((rows, HS), jnp.float32)
    for scale in scales:
        strange = (scale > HIGHEST) | ((scale > 0.0) & (scale < LOWEST))
        odd = jnp.where(strange, 1.0, odd)
        step = jnp.minimum(scale, HIGHEST) * (LIFT / 32767.0)
        noise = noise + step * step * (HS / 12.0)
    scales = [scale * (1.0 / 32767.0) for scale in scales]
    noise = jnp.sum(noise, axis=0, keepdims=True)
    noises = [jnp.where(lane[:1] // SPAN == span, noise[:, span : span + 1], 0.0) for span in range(blocks // SPAN)]
    noise = functools.reduce(jnp.add, noises)
    block_rows = [None] * blocks
    for block in range(half // HS):
        if block % SPAN == 0:
            firsts = (block // SPAN, (block + half // HS) // SPAN)
            steps = [
                [jnp.broadcast_to(scale[:, span : span + 1], (rows, HS)) for span in firsts] for scale in scales
            ]
        totals = [jnp.zeros((rows, HS), jnp.float32)] * 2
        for chunk in range(chunks):
            both = words_ref[chunk, :, pl.ds(block * HS, HS)]
            for nth, code in enumerate((both >> 16, (both << 16) >> 16)):
                totals[nth] = totals[nth] + code.astype(jnp.float32) * steps[chunk][nth]
        for nth, total in enumerate(totals):
            place = block + nth * (half // HS)
            summed_ref[:, pl.ds(place * HS, HS)] = total
            block_rows[place] = jnp.sum(total * total, axis=0, keepdims=True)
    squares = diagonal_row(jnp.concatenate(block_rows, axis=0))
    odd = jnp.sum(odd, axis=0, keepdims=True)
    bad = (noise > (LIFT * NOISE) ** 2 * squares) & (lane[:1] < blocks)
    count = jnp.sum(jnp.where(bad, 1.0, 0.0) + odd, axis=1, keepdims=True)
    out_ref[...] = jnp.broadcast_to(jnp.where(lane[:1] == blocks, count, squares), out_ref.shape)


def kernel(body, out_shape, in_specs, out_specs, flops=None):
    cost = flops and pl.CostEstimate(flops=flops, bytes_accessed=2**19, transcendentals=0)
    return pl.pallas_call(
        body,
        out_shape=out_shape,
        in_specs=in_specs,
        out_specs=out_specs,
        compiler_params=PARAMS,
        cost_estimate=cost,
    )


def to_groups(squares):
    return lax.all_to_all(squares[:, None], GRP, split_axis=0, concat_axis=0, tiled=True)[:, 0]


def exact_sums(own, blocks):
    parts = lax.all_to_all(own, GRP, 0, 0, tiled=True)
    summed = jnp.sum(parts.astype(jnp.float32), axis=0)
    shape = jax.ShapeDtypeStruct((own.shape[0], HS), jnp.float32)
    squares = kernel(functools.partial(squares_body, blocks), shape, [IN_VMEM], IN_VMEM)(summed)
    return summed, squares


def coded_sums(own):
    groups, rows, width = own.shape
    core = lax.axis_index("grp_1")
    pairs = own.reshape(groups // 2, 2, rows, width)
    give = lax.dynamic_index_in_dim(pairs, 1 - core, 1, keepdims=False)
    keep = lax.dynamic_index_in_dim(pairs, core, 1, keepdims=False)
    got = lax.ppermute(give, "grp_1", [(0, 1), (1, 0)])
    sums = keep.astype(jnp.float32) + got.astype(jnp.float32)
    shape = jax.ShapeDtypeStruct((groups // 2, rows, width // 2 + HS), jnp.int32)
    words = kernel(pair_body, shape, [IN_VMEM], IN_VMEM)(sums)
    words = lax.all_to_all(words, "grp_0", 0, 0, tiled=True)
    shapes = (
        jax.ShapeDtypeStruct((rows, width), jnp.float32),
        jax.ShapeDtypeStruct((groups, HS), jnp.float32),
    )
    return kernel(gathered_body, shapes, [IN_VMEM], (IN_VMEM, IN_VMEM))(words)


def shard_exchange(source, occupied, summed, squares):
    rows = summed.shape[0]
    peers = lax.axis_size(SHARD)
    shape = jax.ShapeDtypeStruct((peers * (rows + 1), HS), jnp.int32)
    specs = [IN_SMEM, IN_SMEM, IN_VMEM]
    squares = to_groups(squares)
    packed = kernel(functools.partial(packed_body, peers), shape, specs, IN_VMEM, 4 * 10**6)(source, occupied, summed)
    body = functools.partial(outgoing_body, peers, rows)
    outgoing = kernel(body, shape, [IN_VMEM, IN_VMEM], IN_VMEM)(packed, squares)
    return lax.all_to_all(outgoing[:, None], SHARD, split_axis=0, concat_axis=0, tiled=True)[:, 0]


def unpacked(arrived, wanted, *, blocks, rows, per_peer):
    peers = arrived.shape[0] // (rows + 1)
    shapes = (
        jax.ShapeDtypeStruct((per_peer, peers, rows, HS), jnp.float32),
        jax.ShapeDtypeStruct((per_peer,), jnp.float32),
        jax.ShapeDtypeStruct((3,), jnp.float32),
        jax.ShapeDtypeStruct((1,), jnp.float32),
    )
    body = functools.partial(arrived_body, peers, rows, blocks)
    specs = (IN_VMEM, IN_SMEM, IN_SMEM, IN_SMEM)
    return kernel(body, shapes, [IN_VMEM, IN_VMEM], specs)(arrived, wanted)


def per_device(partial_grads, joined_block, head_slot):
    own_rows = partial_grads[0]
    blocks = joined_block.shape[0]
    groups = lax.axis_size(GRP)
    width = own_rows.shape[1]
    rows = own_rows.shape[0] // groups
    peers = lax.axis_size(SHARD)
    per_peer = (blocks + peers - 1) // peers
    slot_total = per_peer * peers
    first_slot = lax.axis_index(SHARD) * per_peer

    block_ids = jnp.arange(blocks, dtype=jnp.int32)
    slot_ids = jnp.arange(slot_total, dtype=jnp.int32)
    matches = (head_slot[None, :] == slot_ids[:, None]).astype(jnp.int32)
    occupied = jnp.sum(matches, axis=1)
    source = jnp.sum(matches * joined_block[None, :], axis=1)
    block_kind = (block_ids >= QH).astype(jnp.int32) + (block_ids >= QH + KVH).astype(jnp.int32)
    own = head_slot[None, :] == first_slot + jnp.arange(per_peer, dtype=jnp.int32)[:, None]
    alike = block_kind[None, :] == jnp.arange(3, dtype=jnp.int32)[:, None]
    asked = jnp.concatenate([own, alike], axis=0)
    joined = joined_block[:, None] == block_ids[None, :]
    wanted = jnp.any(asked[:, :, None] & joined[None], axis=1).astype(jnp.float32)
    wanted = jnp.pad(wanted, ((0, 8 - wanted.shape[0]), (0, HS - blocks)))

    finish = functools.partial(shard_exchange, source, occupied)
    arrived = finish(*coded_sums(own_rows.reshape(groups, rows, width)))
    unpack = functools.partial(unpacked, wanted=wanted, blocks=blocks, rows=rows, per_peer=per_peer)

    def exactly(state):
        own = jnp.where(state[3][0] > 0.0, own_rows, jnp.zeros_like(own_rows))
        return unpack(finish(*exact_sums(own.reshape(groups, rows, width), blocks)))

    results = lax.while_loop(lambda state: state[3][0] > 0.0, exactly, unpack(arrived))
    return results[:3]


def solution(mesh):
    finer = Mesh(mesh.devices.reshape(8, 2, 4, 8), ("grp_0", "grp_1", "shard_0", "shard_1"))
    in_specs = (P(GRP, SHARD, None), P(), P())
    out_specs = (P(SHARD, None, GRP, None), P(SHARD), P())
    return jax.shard_map(
        per_device, mesh=finer, in_specs=in_specs, out_specs=out_specs, check_vma=False
    )
```
